512 devices in a mesh: groups: 2 (over y), seq: 16 (over z), side: 2 (over core), req: 8 (over x).
Axes of the slice: x: 8, y: 2, z: 16, core: 2. Of those that a mesh axis runs over, the one named last changes fastest.
The devices are a block of a 8x16x16 slice.
Arguments:
- queries: bfloat16 [16, 128, 4, 2048], P(('groups', 'req'), 'seq', 'side'), parts along dimension 0, may hold values from -8 to 8
- cache_keys: bfloat16 [16, 2048, 512], P(('groups', 'req'), 'seq', 'side'), parts along dimension 0, may hold values from -8 to 8
- cache_values: bfloat16 [16, 2048, 512], P(('groups', 'req'), 'seq', 'side'), parts along dimension 0, may hold values from -6 to 6
- tree_keys: bfloat16 [16, 128, 512], P(('groups', 'req'), 'seq', 'side'), parts along dimension 0, may hold values from -8 to 8
- tree_values: bfloat16 [16, 128, 512], P(('groups', 'req'), 'seq', 'side'), parts along dimension 0, may hold values from -6 to 6
- parents: int32 [16, 128], P(('groups', 'req')), parts along dimension 0, may hold values from 0 to 126, as said below
- lengths: int32 [16], P(('groups', 'req')), parts along dimension 0, may hold values from 256 to 2048
- out_weight: bfloat16 [4, 2048, 4096], P('side', 'seq', 'req'), may hold values from -0.0625 to 0.0625
- in_experts: bfloat16 [64, 4096, 1024], P(('seq', 'side'), 'req'), may hold values from -0.09375 to 0.09375
- out_experts: bfloat16 [64, 1024, 4096], P(('seq', 'side'), None, 'req'), may hold values from -0.1875 to 0.1875
- gate_experts: int32 [2048, 8], P(('groups', 'seq', 'side')), parts along dimension 0, may hold values from 0 to 63, all different within a row; in each aligned block of 32 rows (0 to 31, 32 to 63, ...) at most 6 rows name the same one
- gate_weights: float32 [2048, 8], P(('groups', 'seq', 'side')), parts along dimension 0, may hold values from 0.1 to 1
Outputs:
- attended: bfloat16 [2048, 4096], P(('groups', 'seq', 'side'), 'req'), parts along dimension 0
- expert_out: bfloat16 [2048, 4096], P(('groups', 'seq', 'side'), 'req'), parts along dimension 0
The draws below stay inside these ranges and needn't reach their ends.
There are 2 independent parts, one for each index of `groups`. The reference program is written for one: setup_inputs(seed, part) draws one part's arguments, and reference() takes and returns one part's arrays. A program takes and returns all parts, laid end to end along the dimension named above; an argument that names none is the same for every part. Nothing has to cross between parts.
Inputs may be any that keep to these rules, and one draw needn't show every extreme that they name: parents[r, 0] is 0; every node i >= 1 has its parent among nodes i - 4 to i - 1. `gate_experts`: within the 32 rows that one device holds along seq+side, no expert is named by more than 6 rows, and in some such block one expert is named exactly 6 times.
All inputs are finite; a program needn't handle non-finite values.
Results may differ from the reference program's by a relative error of at most 0.018.
Values may be sent and summed in bfloat16 or wider, within the bound.
A program may use at most 128 MiB of HBM per device.

```python
import math
import jax
import jax.numpy as jnp
import numpy as np
from jax import lax

D = 4096
KVH = 4
GROUP = 16
HD = 128
EXPERTS = 64
FF_E = 1024
TOP = 8
CAP = 6
NODES = 128
CTX = 2048
REQS = 8
TOKENS = 1024
TOK_MOE = 32


def draw_queries(key, part):
    shape_all = (REQS, NODES, KVH, GROUP * HD)
    drawn = jnp.clip(1.7 * jax.random.normal(jax.random.fold_in(key, 12), shape_all, jnp.float32), -8.0, 8.0)
    return drawn.astype(jnp.bfloat16)


def draw_cache_keys(key, part):
    shape_all = (REQS, CTX, KVH * HD)
    drawn = jnp.clip(1.7 * jax.random.normal(jax.random.fold_in(key, 22), shape_all, jnp.float32), -8.0, 8.0)
    return drawn.astype(jnp.bfloat16)


def draw_parents(key, part):
    backward = jax.random.randint(jax.random.fold_in(key, 31), (REQS, NODES), 1, 5)
    node_ids = jnp.arange(NODES, dtype=jnp.int32)[None, :]
    return (node_ids - jnp.minimum(backward, node_ids)).astype(jnp.int32)


def plant(values, rng, low, high):
    longest = values.shape.index(max(values.shape))
    spots = []
    for shift in (0, 1):
        where = [jax.random.randint(jax.random.fold_in(rng, axis), (), 0, length) for axis, length in enumerate(values.shape)]
        where[longest] = (where[longest] + shift) % values.shape[longest]
        spots.append(tuple(where))
    return values.at[spots[0]].set(low).at[spots[1]].set(high)


def level_of(rng, dims, shards, low, largest):
    def one(position, shards_of):
        steps = jax.random.uniform(jax.random.fold_in(jax.random.fold_in(rng, 6), position), (shards_of,), jnp.float32, low / len(shards), largest / len(shards))
        return jnp.repeat(jnp.exp(steps), dims[position] // shards_of).reshape((-1,) + (1,) * (len(dims) - position - 1))

    loudness = one(*shards[0])
    for cut in shards[1:]:
        loudness = loudness * one(*cut)
    return loudness


def routed_block(own_key, own, number, rows, number_of, top, bound, slope):
    order = jax.random.permutation(own_key, number_of)
    heavy_load, usual = portions_of(number_of, rows * top, bound, slope, True), portions_of(number_of, rows * top, bound, slope, False)
    places = jnp.arange(number_of)

    def named(tallies, offset_by):
        used = int((tallies > 0).sum())
        fixed = max(1, used // 4)
        shifted = fixed + (places - fixed + offset_by * (used - fixed)) % max(1, number_of - fixed)
        return jnp.zeros((number_of,), jnp.int32).at[order[jnp.where(places < fixed, places, shifted)]].set(jnp.asarray(tallies, jnp.int32))

    tallies = jnp.where(number % 4 == 0, named(heavy_load, number // 4), named(usual, number - number // 4 - 1))
    mixed = jax.random.permutation(jax.random.fold_in(own, 3), number_of)
    giver, receiver = mixed[0:number_of // 2 * 2:2], mixed[1:number_of // 2 * 2:2]
    slack = jnp.minimum(tallies[giver] - 1, bound - tallies[receiver]) // 2
    slack = jnp.where((giver == order[0]) | (receiver == order[0]) | (tallies[receiver] == 0), 0, jnp.maximum(slack, 0))
    shifted = jax.random.randint(jax.random.fold_in(own, 4), (number_of // 2,), 0, 1 << 20) % (slack + 1)
    tallies = tallies.at[giver].add(-shifted).at[receiver].add(shifted)
    items = jnp.searchsorted(jnp.cumsum(tallies), jnp.arange(rows * top), side="right").astype(jnp.int32)
    table = items.reshape(top, rows).T
    table = table[jax.random.permutation(jax.random.fold_in(own, 1), rows)]
    offset_by = jax.random.randint(jax.random.fold_in(own, 2), (rows, 1), 0, top)
    return jnp.take_along_axis(table, (jnp.arange(top)[None, :] + offset_by) % top, axis=1)


def portions_of(count, total, reach, slope, full):
    weights = [(1 << 20) // math.isqrt(rank ** slope) + 1 for rank in range(1, count + 1)]
    largest = reach if full else min(reach, max(-(-total // count), total * weights[0] // sum(weights)))
    least = 1 if total - largest >= count - 1 else 0
    counts, spare = [largest] + [least] * (count - 1), total - largest - least * (count - 1)
    while spare > 0:
        free = [i for i in range(1, count) if counts[i] < largest] or [i for i in range(1, count) if counts[i] < reach]
        mass, remaining = sum([weights[i] for i in free]), spare
        for i in free:
            extra = min(reach - counts[i], max(1, remaining * weights[i] // mass), spare)
            counts[i] = counts[i] + extra
            spare = spare - extra
    return np.array(counts)


def noise(rng, shape, spread, most, pieces=(), held_as=jnp.bfloat16):
    entries = spread * jax.random.normal(rng, shape, jnp.float32)
    if pieces:
        entries = entries * level_of(rng, shape, pieces, -0.22, 0.18)
    return jnp.clip(entries, -most, most).astype(held_as)


def setup_inputs(seed: int = 0, part: int = 0) -> dict:
    streams_of = jax.random.split(jax.random.key(seed), 13)
    part_splits = jax.random.split(jax.random.fold_in(streams_of[12], part), 13)
    queries = draw_queries(jax.random.fold_in(jax.random.fold_in(streams_of[12], part), 71), part)
    cache_keys = draw_cache_keys(jax.random.fold_in(jax.random.fold_in(streams_of[12], part), 71), part)
    cache_values = noise(part_splits[2], (REQS, CTX, KVH * HD), 1.0, 6.0, ((0, 8), (1, 16), (2, 2)))
    tree_keys = noise(part_splits[3], (REQS, NODES, KVH * HD), 1.7, 8.0, ((0, 8), (1, 16), (2, 2)))
    tree_values = noise(part_splits[4], (REQS, NODES, KVH * HD), 1.0, 6.0, ((0, 8), (1, 16), (2, 2)))
    parents = draw_parents(jax.random.fold_in(jax.random.fold_in(streams_of[12], part), 71), part)
    lengths = plant(jax.random.randint(part_splits[6], (REQS,), CTX // 8, CTX + 1), jax.random.fold_in(part_splits[6], 1), CTX // 8, CTX).astype(jnp.int32)
    out_weight = noise(streams_of[7], (KVH, GROUP * HD, D), (KVH * GROUP * HD) ** -0.5, 0.0625, ((0, 2), (1, 16), (2, 8)))
    in_experts = noise(streams_of[8], (EXPERTS, D, FF_E), D ** -0.5, 0.09375, ((0, 32), (1, 8)))
    out_experts = noise(streams_of[9], (EXPERTS, FF_E, D), FF_E ** -0.5, 0.1875, ((0, 32), (2, 8)))
    gate_experts_keys = jax.random.split(jax.random.fold_in(part_splits[10], 1), TOKENS // TOK_MOE)
    gate_experts_turns = jax.random.permutation(jax.random.fold_in(part_splits[10], 3), TOKENS // TOK_MOE)
    gate_experts = jax.vmap(lambda own, number: routed_block(jax.random.fold_in(part_splits[10], 2), own, number, TOK_MOE, EXPERTS, TOP, CAP, 2))(gate_experts_keys, gate_experts_turns).reshape((TOKENS, TOP))
    gate_weights = jnp.clip(jnp.exp(math.log(1.0) - 2.3025851 * jax.random.uniform(part_splits[11], (TOKENS, TOP), jnp.float32) ** level_of(part_splits[11], (TOKENS, TOP), ((0, 32),), -0.2, 0.2)), 0.1, 1.0)
    return {"queries": queries, "cache_keys": cache_keys, "cache_values": cache_values, "tree_keys": tree_keys, "tree_values": tree_values, "parents": parents, "lengths": lengths, "out_weight": out_weight, "in_experts": in_experts, "out_experts": out_experts, "gate_experts": gate_experts, "gate_weights": gate_weights}


def ancestors(parent_row):
    node_ids = jnp.arange(NODES, dtype=jnp.int32)
    parent_hit = (node_ids[None, :] == parent_row[:, None]).astype(jnp.float32)
    reached = jnp.maximum(parent_hit, jnp.eye(NODES, dtype=jnp.float32))
    for turn_number in range(max(1, (NODES - 1).bit_length())):
        reached = jnp.minimum(jnp.dot(reached, reached, precision=lax.Precision.HIGHEST), 1.0)
    return reached

def attend_request(operands):
    query_all, key_cache, value_cache, key_tree, value_tree, parent_row, length = operands
    reached = ancestors(parent_row)
    context_seen = jnp.arange(CTX, dtype=jnp.int32) < length
    visible = jnp.concatenate([jnp.broadcast_to(context_seen[None, :], (NODES, CTX)), reached > 0.5], axis=1)
    factor = 1.0 / math.sqrt(HD)
    results = []
    for head_pair in range(KVH):
        first_col = head_pair * HD
        key_rows = jnp.concatenate([key_cache[:, first_col:first_col + HD], key_tree[:, first_col:first_col + HD]], axis=0).astype(jnp.float32)
        value_rows = jnp.concatenate([value_cache[:, first_col:first_col + HD], value_tree[:, first_col:first_col + HD]], axis=0).astype(jnp.float32)
        query_block = query_all[:, head_pair].reshape(NODES, GROUP, HD).astype(jnp.float32)
        scores = jnp.einsum('ngd,kd->ngk', query_block, key_rows, precision=lax.Precision.HIGHEST) * factor
        scores = jnp.where(visible[:, None, :], scores, -jnp.inf)
        weights = jax.nn.softmax(scores, axis=-1)
        weights_low = lax.optimization_barrier(weights.astype(jnp.bfloat16)).astype(jnp.float32)
        results.append(jnp.einsum('ngk,kd->ngd', weights_low, value_rows, precision=lax.Precision.HIGHEST))
    return jnp.stack(results, axis=1)

def reference(queries, cache_keys, cache_values, tree_keys, tree_values, parents, lengths, out_weight, in_experts, out_experts, gate_experts, gate_weights):
    attention = lax.map(attend_request, (queries, cache_keys, cache_values, tree_keys, tree_values, parents, lengths))
    attention = attention.reshape(REQS * NODES, KVH * GROUP * HD).astype(jnp.bfloat16)
    projector = out_weight.reshape(KVH * GROUP * HD, D).astype(jnp.float32)
    attended = jnp.dot(attention.astype(jnp.float32), projector, precision=lax.Precision.HIGHEST).astype(jnp.bfloat16)
    token_count = REQS * NODES
    limit = token_count // TOK_MOE * CAP
    token_ids = jnp.arange(token_count, dtype=jnp.int32)

    def add_expert(carry, expert_id):
        chosen = gate_experts == expert_id
        coefficient = lax.optimization_barrier(jnp.sum(jnp.where(chosen, gate_weights, 0.0), axis=1))
        user = jnp.any(chosen, axis=1)
        order = jnp.argsort(jnp.where(user, 0, 1).astype(jnp.int32) * token_count + token_ids)[:limit].astype(jnp.int32)
        row_block = attended[order].astype(jnp.float32)
        before = jnp.dot(row_block, in_experts[expert_id].astype(jnp.float32), precision=lax.Precision.HIGHEST)
        hidden = jax.nn.silu(before).astype(jnp.bfloat16)
        produced = jnp.dot(hidden.astype(jnp.float32), out_experts[expert_id].astype(jnp.float32), precision=lax.Precision.HIGHEST).astype(jnp.bfloat16)
        produced = lax.optimization_barrier(produced).astype(jnp.float32)
        return (carry.at[order].add(coefficient[order][:, None] * produced), None)
    summed, unused_rows = lax.scan(add_expert, jnp.zeros((token_count, D), jnp.float32), jnp.arange(EXPERTS, dtype=jnp.int32))
    return (attended, summed.astype(jnp.bfloat16))
```

```python
import functools
import math

import jax
import jax.numpy as jnp
from jax import lax
from jax.experimental import pallas as pl
from jax.experimental.pallas import tpu as pltpu
from jax.sharding import PartitionSpec as P

HD = 128
CAP = 6
NEG_FILL = -1e30
F32 = jnp.float32
BF16 = jnp.bfloat16
MESH = pl.DeviceIdType.MESH
MINUS, PLUS = 0, 1


def nt(a, b):
    return lax.dot_general(a, b, (((1,), (1,)), ((), ())), preferred_element_type=F32)


def nn(a, b):
    return lax.dot_general(a, b, (((1,), (0,)), ((), ())), preferred_element_type=F32)


def steps_of(n, j, way):
    short = (j + way) % 2
    return n // 2 - short


class Ring:
    def __init__(self, axis, n, me, send_sem, recv_sem, started):
        self.axis, self.n, self.me = axis, n, me
        self.send_sem, self.recv_sem, self.started = send_sem, recv_sem, started

    def at(self, offset):
        return lax.rem(self.me + (offset + self.n) % self.n, self.n)

    def copy(self, src, dst, j, way, s):
        return pltpu.make_async_remote_copy(
            src_ref=src,
            dst_ref=dst,
            send_sem=self.send_sem.at[j, way, s],
            recv_sem=self.recv_sem.at[j, way, s],
            device_id={self.axis: self.at(-1 if way == MINUS else 1)},
            device_id_type=MESH,
        )

    def send(self, src, dst, j, way, s):
        c = self.copy(src, dst, j, way, s)
        c.start()
        self.started.append(c)

    def arrived(self, ref, j, way, s):
        self.copy(ref, ref, j, way, s).wait_recv()


class Gather(Ring):
    def set(self, views):
        self.views = views
        return self

    def source(self, way, s):
        return self.at(s if way == MINUS else -s)

    def forward(self, j, way, s):
        if s < steps_of(self.n, j, way):
            ref = self.views[j](self.source(way, s))
            self.send(ref, ref, j, way, s)

    def begin(self, j):
        for way in (MINUS, PLUS):
            self.forward(j, way, 0)

    def take(self, j, way, s):
        if s > steps_of(self.n, j, way):
            return None
        p = self.source(way, s)
        self.arrived(self.views[j](p), j, way, s - 1)
        self.forward(j, way, s)
        return p


def kernel(
    cfg,
    q_hbm, k_hbm, v_hbm, t_hbm, gate_hbm, w_hbm, win_hbm, wout_hbm, par_ref, len_ref,
    att_out, exp_out,
    kv, gbuf, qbuf, qmat, wb, win, wout, reach_ref, m_ref, l_ref, acc_ref, att, abuf, part,
    rs_out, rs_in, xall, hit_ref, wsel_ref, pmat, pt, wrow, rows, hs_out, hs_in, hbuf, prod, sib_out, sib_in,
    rt_out, rt_in,
    load_sem, q_s, q_r, kv_s, kv_r, sib_s, sib_r, xa_s, xa_r, rs_s, rs_r, ag_s, ag_r, sx_s, sx_r,
    hr_s, hr_r, hg_s, hg_r, rt_s, rt_r,
):
    nz, nx, kvl, nl, tb, zpr, top, el, sl = cfg
    z, side, x = lax.axis_index("seq"), lax.axis_index("side"), lax.axis_index("req")
    other = 1 - side
    nodes = nz * nl
    sent = []

    loads = []

    def load(src, dst):
        c = pltpu.make_async_copy(src, dst, load_sem.at[len(loads)])
        c.start()
        loads.append(c)

    ctx = k_hbm.shape[0]
    tr = t_hbm.shape[0]
    load(q_hbm, qbuf.at[0])
    load(k_hbm, kv.at[z, pl.ds(0, ctx)])
    load(t_hbm, kv.at[z, pl.ds(ctx, tr)])
    load(v_hbm, kv.at[z, pl.ds(ctx + tr, ctx)])
    load(gate_hbm, gbuf.at[side, z])
    load(w_hbm, wb.at[side])
    load(win_hbm, win)
    load(wout_hbm, wout)

    barrier = pltpu.get_barrier_semaphore()
    peers = [{"seq": lax.rem(z + d, nz)} for d in range(1, nz)]
    peers += [{"req": lax.rem(x + d, nx)} for d in sorted({1, nx - 1})]
    peers += [{"side": other}]
    for peer in peers:
        pl.semaphore_signal(barrier, inc=1, device_id=peer, device_id_type=MESH)
    pl.semaphore_wait(barrier, len(peers))

    def sibling(src, dst, i):
        return pltpu.make_async_remote_copy(
            src_ref=src, dst_ref=dst, send_sem=sib_s.at[i], recv_sem=sib_r.at[i],
            device_id={"side": other}, device_id_type=MESH,
        )

    def sibling_send(src, dst, i):
        c = sibling(src, dst, i)
        c.start()
        sent.append(c)

    loads[0].wait()
    for d in range(1, nz):
        to = lax.rem(z + d, nz)
        c = pltpu.make_async_remote_copy(
            src_ref=qbuf.at[0, to], dst_ref=qbuf.at[1, z], send_sem=q_s.at[d - 1], recv_sem=q_r.at[d - 1],
            device_id={"seq": to}, device_id_type=MESH,
        )
        c.start()
        sent.append(c)
    views = [
        lambda p: kv.at[p, pl.ds(0, ctx + tr)],
        lambda p: kv.at[p, pl.ds(ctx + tr, ctx)],
        lambda p: gbuf.at[side, p],
    ]
    ring = Gather("seq", nz, z, kv_s, kv_r, sent).set(views)
    loads[1].wait()
    loads[2].wait()
    ring.begin(0)
    loads[3].wait()
    ring.begin(1)
    loads[4].wait()
    ring.begin(2)
    loads[5].wait()
    sibling_send(wb.at[side], wb.at[side], 0)

    row_i = lax.broadcasted_iota(jnp.int32, (nodes, nodes), 0)
    col_i = lax.broadcasted_iota(jnp.int32, (nodes, nodes), 1)
    eye = jnp.where(row_i == col_i, 1.0, 0.0)
    back = jnp.maximum(jnp.where(row_i == par_ref[...], 1.0, 0.0), eye)
    for turn in range(max(1, (nodes - 1).bit_length())):
        low = back.astype(BF16)
        back = jnp.minimum(nn(low, low), 1.0)
    reach = nt(eye.astype(BF16), back.astype(BF16)).astype(BF16)
    spread_row = lax.broadcasted_iota(jnp.int32, (nodes, nz * tr), 0)
    spread_col = lax.broadcasted_iota(jnp.int32, (nodes, nz * tr), 1)
    spread = jnp.where(spread_col == (spread_row // nl) * tr + lax.rem(spread_row, nl), 1.0, 0.0)
    reach_ref[...] = nn(reach, spread.astype(BF16))

    for d in range(1, nz):
        frm = lax.rem(z + nz - d, nz)
        pltpu.make_async_remote_copy(
            src_ref=qbuf.at[0, frm], dst_ref=qbuf.at[1, frm], send_sem=q_s.at[d - 1], recv_sem=q_r.at[d - 1],
            device_id={"seq": frm}, device_id_type=MESH,
        ).wait_recv()
    qbuf[1, z] = qbuf[0, z]
    q_all = qbuf[1].astype(F32).reshape(nz, kvl, nl, HD)
    for c in range(kvl):
        qmat[c] = q_all[:, c].reshape(nodes, HD).astype(BF16)
    factor = 1.0 / math.sqrt(HD)
    m_ref[...] = jnp.full_like(m_ref, NEG_FILL)
    l_ref[...] = jnp.zeros_like(l_ref)
    acc_ref[...] = jnp.zeros_like(acc_ref)

    def absorb(c, keys, seen, values, shift):
        scores = jnp.where(seen, nt(qmat[c], keys) * factor, NEG_FILL)
        old = m_ref[c]
        new = jnp.maximum(old, jnp.max(scores, axis=1, keepdims=True))
        weights = jnp.where(seen, jnp.exp(scores - new), 0.0)
        scale = jnp.exp(old - new)
        m_ref[c] = new
        l_ref[c] = l_ref[c] * scale + jnp.sum(weights, axis=1, keepdims=True)
        if shift:
            weights = pltpu.roll(weights, shift, 1)
        acc_ref[c] = acc_ref[c] * scale + nn(weights.astype(BF16), values)

    length = len_ref[0]
    key_pos = lax.broadcasted_iota(jnp.int32, (nodes, ctx), 1)

    def attend(p):
        seen = key_pos + p * ctx < length
        for c in range(kvl):
            lanes = slice(c * HD, (c + 1) * HD)
            absorb(c, kv[p, 0:ctx, lanes], seen, kv[p, ctx + tr : 2 * ctx + tr, lanes], 0)

    attend(z)
    for s in range(1, nz // 2 + 1):
        got = [[ring.take(j, way, s) for j in range(3)] for way in (MINUS, PLUS)]
        if s < nz // 2:
            attend(got[MINUS][0])
            attend(got[PLUS][0])
        else:
            attend(got[MINUS][0])
    sibling_send(gbuf.at[side], gbuf.at[side], 1)

    for c in range(kvl):
        lanes = slice(c * HD, (c + 1) * HD)
        tree = kv[:, ctx : ctx + tr, lanes].reshape(nz * tr, HD)
        absorb(c, tree, reach_ref[...] > 0.5, tree, nl)
        att[:, :, lanes] = (acc_ref[c] / l_ref[c]).astype(BF16).reshape(zpr * 2, tb, HD)

    for h in range(zpr):
        sibling_send(att.at[2 * h + other], abuf.at[x, side, h], 2 + h)
    for h in range(zpr):
        abuf[x, side, h] = att[2 * h + side]
    ring = Gather("req", nx, x, xa_s, xa_r, sent).set([lambda p: abuf.at[p, side], lambda p: abuf.at[p, other]])
    ring.begin(0)
    for h in range(zpr):
        sibling(att.at[2 * h + other], abuf.at[x, other, h], 2 + h).wait_recv()
    ring.begin(1)
    sibling(wb.at[side], wb.at[other], 0).wait_recv()

    def project(r):
        a0 = abuf[r, 0].reshape(zpr * tb, kvl * HD)
        a1 = abuf[r, 1].reshape(zpr * tb, kvl * HD)
        part[pl.ds(r * zpr, zpr)] = (nn(a0, wb[0]) + nn(a1, wb[1])).reshape(zpr, tb, -1)

    project(x)
    for s in range(1, nx // 2 + 1):
        got = [[ring.take(j, way, s) for j in range(2)] for way in (MINUS, PLUS)]
        if s < nx // 2:
            project(got[MINUS][0])
            project(got[PLUS][0])
        else:
            project(got[MINUS][0])

    def reduce_scatter(ring, out, inn, own, chunks):
        n = ring.n

        def put(j, way, s):
            steps = steps_of(n, j, way)
            if s >= steps:
                return
            left = steps - s
            value = own(ring.at(-left if way == MINUS else left), j)
            if s > 0:
                ring.arrived(inn.at[j, way, s - 1], j, way, s - 1)
                value = value + inn[j, way, s - 1].astype(F32)
            out[j, way, s] = value.astype(BF16)
            ring.send(out.at[j, way, s], inn.at[j, way, s], j, way, s)

        for s in range(n // 2):
            for j in range(chunks):
                for way in (MINUS, PLUS):
                    put(j, way, s)

        def total(j):
            value = own(ring.me, j)
            for way in (MINUS, PLUS):
                steps = steps_of(n, j, way)
                if steps:
                    ring.arrived(inn.at[j, way, steps - 1], j, way, steps - 1)
                    value = value + inn[j, way, steps - 1].astype(F32)
            return value

        return total

    half = tb // 2
    ring = Ring("seq", nz, z, rs_s, rs_r, sent)
    total = reduce_scatter(ring, rs_out, rs_in, lambda p, j: part[p, pl.ds(j * half, half), :], 2)
    ring = Gather("seq", nz, z, ag_s, ag_r, sent).set(
        [functools.partial(lambda j, p: xall.at[p, side, pl.ds(j * half, half)], j) for j in range(2)]
    )

    def across(j, way, s, p, whose):
        ref = xall.at[p, whose, pl.ds(j * half, half)]
        return pltpu.make_async_remote_copy(
            src_ref=ref, dst_ref=ref, send_sem=sx_s.at[j, way, s], recv_sem=sx_r.at[j, way, s],
            device_id={"side": other}, device_id_type=MESH,
        )

    def hand_over(j, way, s, p):
        c = across(j, way, s, p, side)
        c.start()
        sent.append(c)

    for j in range(2):
        xall[z, side, pl.ds(j * half, half)] = total(j).astype(BF16)
        ring.begin(j)
        hand_over(j, MINUS, 0, z)
    att_out[...] = xall[z, side]

    sibling(gbuf.at[side], gbuf.at[other], 1).wait_recv()
    upper = jnp.where(row_i <= col_i, 1.0, 0.0).astype(BF16)
    slot_i = lax.broadcasted_iota(jnp.int32, (sl, nodes), 0).astype(F32)
    first = ((z * 2 + side) * el + 1).astype(F32)
    for r in range(nx):
        gates = jnp.zeros((2 * top, nodes), F32)
        for h in range(zpr):
            for w in range(2):
                gates = gates + gbuf[w, r * zpr + h].astype(F32)
        for e in range(el):
            match = jnp.where(gates[:top] == first + e, 1.0, 0.0)
            hit_ref[e, r : r + 1] = jnp.sum(match, axis=0, keepdims=True)
            wsel_ref[e, r : r + 1] = jnp.sum(match * gates[top:], axis=0, keepdims=True)
    for e in range(el):
        hits = hit_ref[e]
        ranks = nn(hits.astype(BF16), upper)
        before = jnp.zeros((1, 1), F32)
        total_w = jnp.zeros((sl, 1), F32)
        for r in range(nx):
            slot = jnp.where(hits[r : r + 1] > 0.5, ranks[r : r + 1] + before - 1.0, -1.0)
            place = jnp.where(slot_i == slot, 1.0, 0.0)
            total_w = total_w + jnp.sum(place * wsel_ref[e, r : r + 1], axis=1, keepdims=True)
            pmat[pl.ds(e * sl, sl), r * nodes : (r + 1) * nodes] = place.astype(BF16)
            before = before + ranks[r : r + 1, nodes - 1 :]
        wrow[pl.ds(e * sl, sl)] = total_w
    eye_low = eye.astype(BF16)
    for r in range(nx):
        pt[pl.ds(r * nodes, nodes)] = nt(eye_low, pmat[:, r * nodes : (r + 1) * nodes]).astype(BF16)

    for s in range(1, nz // 2 + 1):
        for j in range(2):
            for way in (MINUS, PLUS):
                p = ring.take(j, way, s)
                if p is not None:
                    hand_over(j, way, s, p)
    for s in range(nz // 2 + 1):
        for j in range(2):
            for way in (MINUS, PLUS):
                if s <= steps_of(nz, j, way) and (s or way == MINUS):
                    across(j, way, s, ring.source(way, s), other).wait_recv()

    tokens = nz * 2 * tb
    flat = xall[...].reshape(tokens, xall.shape[-1])
    for e in range(el):
        rows[e] = nn(pmat[pl.ds(e * sl, sl)], flat).astype(BF16)
    loads[6].wait()
    hb = hbuf.shape[-1]
    ring = Ring("req", nx, x, hr_s, hr_r, sent)
    total = reduce_scatter(
        ring, hs_out, hs_in,
        lambda p, e: nn(rows[e], win[e, :, pl.ds(pl.multiple_of(p * hb, hb), hb)]), el,
    )
    ring = Gather("req", nx, x, hg_s, hg_r, sent).set(
        [functools.partial(lambda e, p: hbuf.at[p, e], e) for e in range(el)]
    )
    for e in range(el):
        value = total(e)
        hbuf[x, e] = (value / (1.0 + jnp.exp(-value))).astype(BF16)
        ring.begin(e)
    loads[7].wait()

    def produce(p, e):
        return nn(hbuf[p, e], wout[e, pl.ds(pl.multiple_of(p * hb, hb), hb), :])

    for e in range(el):
        prod[e] = produce(x, e)
    for s in range(1, nx // 2 + 1):
        for e in range(el):
            for way in (MINUS, PLUS):
                p = ring.take(e, way, s)
                if p is not None:
                    prod[e] = prod[e] + produce(p, e)
    for e in range(el):
        rows[e] = (prod[e] * wrow[pl.ds(e * sl, sl)]).astype(BF16)
    made = rows[...].reshape(el * sl, -1)
    for r in range(nx):
        mixed = nn(pt[pl.ds(r * nodes, nodes)], made).reshape(zpr, 2, tb, -1)
        for h in range(zpr):
            for w in range(2):
                @pl.when(side == w)
                def _():
                    part[r * zpr + h] = mixed[h, w]

                @pl.when(side != w)
                def _():
                    sib_out[r * zpr + h] = mixed[h, w].astype(BF16)
    sibling_send(sib_out, sib_in, 2 + zpr)
    sibling(sib_out, sib_in, 2 + zpr).wait_recv()
    ring = Ring("seq", nz, z, rt_s, rt_r, sent)
    total = reduce_scatter(
        ring, rt_out, rt_in,
        lambda p, j: part[p, pl.ds(j * half, half), :] + sib_in[p, pl.ds(j * half, half), :].astype(F32), 2,
    )
    for j in range(2):
        exp_out[pl.ds(j * half, half)] = total(j).astype(BF16)
    for c in sent:
        c.wait_send()


def per_device(
    queries, cache_keys, cache_values, tree_keys, tree_values, parents, lengths,
    out_weight, in_experts, out_experts, gate_experts, gate_weights,
):
    nz, nx = lax.axis_size("seq"), lax.axis_size("req")
    sides = lax.axis_size("side")
    _, nl, kvl, gd = queries.shape
    ctx, width = cache_keys.shape[1], cache_keys.shape[2]
    tb, top = gate_experts.shape
    el, feats, ff = in_experts.shape
    zpr = nz // nx
    nodes = nz * nl
    sl = nz * sides * CAP
    hb = ff // nx
    half = tb // 2
    cols = out_weight.shape[2]

    q = queries[0].reshape(nl, kvl, nz, HD).transpose(2, 1, 0, 3).reshape(nz, kvl * nl, HD)
    tree = jnp.concatenate([tree_keys[0], tree_values[0]], axis=0)
    place = lax.rem(lax.axis_index("seq") * sides + lax.axis_index("side"), zpr * sides)
    both = jnp.concatenate([(gate_experts + 1).astype(F32), gate_weights], axis=1).T
    lane = jnp.arange(nodes, dtype=jnp.int32)[None, :]
    gates = jnp.where(lane // tb == place, jnp.tile(both, (1, zpr * sides)), 0.0).astype(BF16)
    wide = out_weight.reshape(kvl * HD, cols)

    cfg = (nz, nx, kvl, nl, tb, zpr, top, el, sl)
    any_spec = pl.BlockSpec(memory_space=pl.ANY)
    vmem_spec = pl.BlockSpec(memory_space=pltpu.VMEM)
    hz, hx = nz // 2, nx // 2
    dma = pltpu.SemaphoreType.DMA
    V = pltpu.VMEM
    tr = 2 * nl
    scratch = [
        V((nz, 2 * ctx + tr, width), BF16),
        V((2, nz, 2 * top, nodes), BF16),
        V((2, nz, kvl * nl, HD), BF16),
        V((kvl, nodes, HD), BF16),
        V((2, kvl * HD, cols), BF16),
        V((el, feats, ff), BF16),
        V((el, ff, cols), BF16),
        V((nodes, nz * tr), F32),
        V((kvl, nodes, 1), F32),
        V((kvl, nodes, 1), F32),
        V((kvl, nodes, HD), F32),
        V((zpr * 2, tb, kvl * HD), BF16),
        V((nx, 2, zpr, tb, kvl * HD), BF16),
        V((nz, tb, cols), F32),
        V((2, 2, hz, half, cols), BF16),
        V((2, 2, hz, half, cols), BF16),
        V((nz, 2, tb, cols), BF16),
        V((el, nx, nodes), F32),
        V((el, nx, nodes), F32),
        V((el * sl, nx * nodes), BF16),
        V((nx * nodes, el * sl), BF16),
        V((el * sl, 1), F32),
        V((el, sl, cols), BF16),
        V((el, 2, hx, sl, hb), BF16),
        V((el, 2, hx, sl, hb), BF16),
        V((nx, el, sl, hb), BF16),
        V((el, sl, cols), F32),
        V((nz, tb, cols), BF16),
        V((nz, tb, cols), BF16),
        V((2, 2, hz, half, cols), BF16),
        V((2, 2, hz, half, cols), BF16),
        dma((8,)),
        dma((nz - 1,)), dma((nz - 1,)),
        dma((3, 2, hz)), dma((3, 2, hz)),
        dma((3 + zpr,)), dma((3 + zpr,)),
        dma((2, 2, hx)), dma((2, 2, hx)),
        dma((2, 2, hz)), dma((2, 2, hz)),
        dma((2, 2, hz)), dma((2, 2, hz)),
        dma((2, 2, hz + 1)), dma((2, 2, hz + 1)),
        dma((el, 2, hx)), dma((el, 2, hx)),
        dma((el, 2, hx)), dma((el, 2, hx)),
        dma((2, 2, hz)), dma((2, 2, hz)),
    ]
    block = jax.ShapeDtypeStruct((tb, cols), BF16)
    return pl.pallas_call(
        functools.partial(kernel, cfg),
        out_shape=(block, block),
        in_specs=[any_spec] * 8 + [vmem_spec, pl.BlockSpec(memory_space=pltpu.SMEM)],
        out_specs=(vmem_spec, vmem_spec),
        scratch_shapes=scratch,
        compiler_params=pltpu.CompilerParams(
            collective_id=0, has_side_effects=True, vmem_limit_bytes=48 * 1024 * 1024
        ),
    )(q, cache_keys[0], cache_values[0], tree, gates, wide, in_experts, out_experts, parents, lengths)


def solution(mesh):
    placed = (
        P(("groups", "req"), "seq", "side", None),
        P(("groups", "req"), "seq", "side"),
        P(("groups", "req"), "seq", "side"),
        P(("groups", "req"), "seq", "side"),
        P(("groups", "req"), "seq", "side"),
        P(("groups", "req"), None),
        P(("groups", "req")),
        P("side", "seq", "req"),
        P(("seq", "side"), "req", None),
        P(("seq", "side"), None, "req"),
        P(("groups", "seq", "side"), None),
        P(("groups", "seq", "side"), None),
    )
    return jax.shard_map(
        per_device,
        mesh=mesh,
        in_specs=placed,
        out_specs=(P(("groups", "seq", "side"), "req"), P(("groups", "seq", "side"), "req")),
        check_vma=False,
    )
```
